32 devices in a mesh: seq: 8 (over z, y), mp: 4 (over x, core).
Axes of the slice: x: 2, y: 2, z: 4, core: 2. Of those that a mesh axis runs over, the one named last changes fastest.
Arguments:
- gate_in: bfloat16 [8192, 1024], P('seq', 'mp'), may hold values from -5 to 5
- value_in: bfloat16 [8192, 1024], P('seq', 'mp'), may hold values from -5 to 5
- out_gate: bfloat16 [8192, 1024], P('seq', 'mp'), may hold values from -10 to 10
- filter_taps: bfloat16 [4096, 1024], P('seq', 'mp'), may hold values from -0.09375 to 0.09375
- skip_gain: float32 [1024], P('mp'), may hold values from -4 to 4
Outputs:
- output: bfloat16 [8192, 1024], P('seq', 'mp')
The draws below stay inside these ranges and needn't reach their ends.
All inputs are finite; a program needn't handle non-finite values.
Results may differ from the reference program's by a relative error of at most 0.009.
Values may be sent and summed in bfloat16 or wider, within the bound.
A program may use at most 64 MiB of HBM per device.

```python
import math
import jax
import jax.numpy as jnp
from jax import lax

C = 1024
K = 4096
TOKENS = 8192


def draw_out_gate(key, part):
    first_key, second_key = jax.random.split(jax.random.fold_in(key, 11), 2)
    position = jnp.arange(C, dtype=jnp.float32) / (C - 1)
    ramp = 0.55 * jnp.power(3.0, position)
    channel_scale = jnp.exp(jax.random.uniform(second_key, (C,), jnp.float32, math.log(0.7), math.log(1.4)))
    base = jnp.clip(jax.random.normal(first_key, (TOKENS, C), jnp.float32), -4.0, 4.0)
    return (base * ramp[None, :] * channel_scale[None, :]).astype(jnp.bfloat16)


def block_scale(key, dims, pieces, smallest, largest):
    def one(dim, parts):
        draws = jax.random.uniform(jax.random.fold_in(jax.random.fold_in(key, 6), dim), (parts,), jnp.float32, smallest / len(pieces), largest / len(pieces))
        return jnp.repeat(jnp.exp(draws), dims[dim] // parts).reshape((-1,) + (1,) * (len(dims) - dim - 1))

    loudness = one(*pieces[0])
    for cut in pieces[1:]:
        loudness = loudness * one(*cut)
    return loudness


def gaussian(stream_key, extent, scale, bound, cuts=(), held_as=jnp.bfloat16):
    loudness = block_scale(stream_key, extent, cuts, -0.22, 0.18) if cuts else 1.0
    entries = jax.random.normal(stream_key, extent, jnp.float32) * scale * loudness
    return jnp.minimum(jnp.maximum(entries, -bound), bound).astype(held_as)


def setup_inputs(seed: int = 0) -> dict:
    keys = jax.random.split(jax.random.key(seed), 6)
    return {
        "gate_in": gaussian(keys[0], (TOKENS, C), 1.0, 5.0, ((0, 8), (1, 4))),
        "value_in": gaussian(keys[1], (TOKENS, C), 1.0, 5.0, ((0, 8), (1, 4))),
        "out_gate": draw_out_gate(jax.random.fold_in(keys[5], 71), 0),
        "filter_taps": gaussian(keys[3], (K, C), K ** -0.5, 0.09375, ((0, 8), (1, 4))),
        "skip_gain": gaussian(keys[4], (C,), 1.0, 4.0, ((0, 4),), jnp.float32),
    }


def convolve_group(signal_kernel):
    signal, kernel = signal_kernel
    length = signal.shape[1]
    size = 1 << (length + kernel.shape[1] - 1).bit_length()
    product = jnp.fft.rfft(signal, size) * jnp.fft.rfft(kernel, size)
    return jnp.fft.irfft(product, size)[:, :length]

def reference(gate_in, value_in, out_gate, filter_taps, skip_gain):
    gated = (gate_in.astype(jnp.float32) * value_in.astype(jnp.float32)).astype(jnp.bfloat16)
    group = 32
    signal = gated.astype(jnp.float32).T.reshape(C // group, group, TOKENS)
    kernel = filter_taps.astype(jnp.float32).T.reshape(C // group, group, K)
    convolved = lax.map(convolve_group, (signal, kernel)).reshape(C, TOKENS).T
    mixed = out_gate.astype(jnp.float32) * (convolved + skip_gain[None, :] * gated.astype(jnp.float32))
    power = lax.optimization_barrier(jnp.mean(mixed * mixed, axis=1, keepdims=True))
    return (mixed / jnp.sqrt(power + 1e-05)).astype(jnp.bfloat16)
```

```python
import functools

import jax
import jax.numpy as jnp
from jax import lax
from jax.experimental import pallas as pl
from jax.experimental.pallas import tpu as pltpu
from jax.sharding import PartitionSpec as P

MESH = pl.DeviceIdType.MESH
LANES = 128
TAPS, GATED, RESULT = 0, 1, 2
EPS = 1e-05


def peer_of(me, k, n):
    if n & (n - 1) == 0:
        return me ^ k
    return lax.rem(me + k, n)


def source_of(me, k, n):
    if n & (n - 1) == 0:
        return me ^ k
    return lax.rem(me + n - k, n)


def kernel(cfg, gate, value, og, taps, skip, out, stage, xm, hm, xr, hr, hf, xpad, rs, cr, ogt,
           mixed, power, powers, send_sem, recv_sem, own_sem, psend_sem, precv_sem):
    n, m, channels, blocks, cl, width, groups, sent_taps, hs, he, total_c = cfg
    me = lax.axis_index("seq")
    mine = lax.axis_index("mp")
    nd = hs * he
    order = list(range(n - 1, 0, -1))

    barrier = pltpu.get_barrier_semaphore()
    for k in range(1, n):
        pl.semaphore_signal(barrier, inc=1, device_id={"seq": peer_of(me, k, n)}, device_id_type=MESH)
    for k in range(1, m):
        pl.semaphore_signal(barrier, inc=1, device_id={"mp": peer_of(mine, k, m)}, device_id_type=MESH)

    if sent_taps:
        for e in range(he):
            part = taps[e * LANES:(e + 1) * LANES, :].astype(jnp.float32)
            stage[pl.ds(e, channels, stride=he), :] = part.T
        hm[...] = stage[: channels * he, :].astype(jnp.bfloat16).reshape(hm.shape)
    for a in range(blocks):
        span = slice(a * LANES, (a + 1) * LANES)
        part = gate[span, :].astype(jnp.float32) * value[span, :].astype(jnp.float32)
        stage[pl.ds(a, channels, stride=blocks), :] = part.T
    xm[...] = stage[...].astype(jnp.bfloat16).reshape(xm.shape)

    pl.semaphore_wait(barrier, n - 1 + m - 1)

    def rows_of(kind, g):
        per = he if kind == TAPS else blocks
        return pl.ds(g * width * per, width * per)

    def refs(kind):
        return {TAPS: (hm, hr), GATED: (xm, xr), RESULT: (rs, cr)}[kind]

    def remote(kind, g, k):
        src, dst = refs(kind)
        to = peer_of(me, k, n)
        rows = rows_of(kind, g)
        return pltpu.make_async_remote_copy(
            src_ref=src.at[to, rows],
            dst_ref=dst.at[me, rows],
            send_sem=send_sem.at[kind, g, k],
            recv_sem=recv_sem.at[kind, g, k],
            device_id={"seq": to},
            device_id_type=MESH,
        )

    def arrival(kind, g, k):
        src, dst = refs(kind)
        whence = source_of(me, k, n)
        rows = rows_of(kind, g)
        return pltpu.make_async_remote_copy(
            src_ref=src.at[whence, rows],
            dst_ref=dst.at[whence, rows],
            send_sem=send_sem.at[kind, g, k],
            recv_sem=recv_sem.at[kind, g, k],
            device_id={"seq": whence},
            device_id_type=MESH,
        )

    def own(kind, g):
        src, dst = refs(kind)
        rows = rows_of(kind, g)
        return pltpu.make_async_copy(src.at[me, rows], dst.at[me, rows], own_sem.at[kind, g])

    forward = ([TAPS] if sent_taps else []) + [GATED]
    for g in range(groups):
        for kind in forward:
            for k in order:
                remote(kind, g, k).start()
            own(kind, g).start()

    for a in range(blocks):
        span = slice(a * LANES, (a + 1) * LANES)
        ogt[pl.ds(a, channels, stride=blocks), :] = og[span, :].astype(jnp.float32).T
    xpad[:, :nd, :] = jnp.zeros((2, nd, LANES), jnp.float32)

    lane = lax.broadcasted_iota(jnp.int32, (16, LANES), 1)
    sub = lax.broadcasted_iota(jnp.int32, (16, LANES), 0)
    total = n * blocks

    def toeplitz(c):
        lines = []
        for d in range(nd):
            source = hf if sent_taps else taps
            line = source[d // he, pl.ds(c * he + d % he, 1), :]
            line = jnp.broadcast_to(line, (16, LANES))
            lines.append(pltpu.roll(line, 0, 1, stride=1, stride_axis=0))
        zero = jnp.zeros((16, LANES), jnp.float32)
        first = []
        for d in range(nd + 1):
            here = lines[d] if d < nd else zero
            before = lines[d - 1] if d > 0 else zero
            first.append(jnp.where(lane >= sub, here, before))
        tiles = []
        turned = [[(f if q == 0 else pltpu.roll(f, 16 * q, 1)) for q in range(8)] for f in first]
        for d in range(nd + 1):
            rows = []
            for q in range(8):
                before = turned[d - 1][q] if d > 0 else zero
                rows.append(turned[d][q] if q == 0 else jnp.where(lane >= 16 * q, turned[d][q], before))
            tiles.append(jnp.concatenate(rows, axis=0).astype(jnp.bfloat16))
        return tiles

    def one_pair(base, p):
        c0 = base + 2 * p
        start = pl.multiple_of(c0 * blocks, 2 * blocks)
        both = xr[:, pl.ds(start, 2 * blocks), :].astype(jnp.float32)
        results = []
        for e in range(2):
            rows = both[:, e * blocks:(e + 1) * blocks, :].reshape(total, LANES)
            xpad[e, nd:, :] = rows
            tiles = toeplitz(c0 + e)
            acc = rows * skip[me * cl + c0 + e]
            for d in range(0, nd + 1, 2):
                ds = [d, d + 1] if d + 1 <= nd else [d]
                left = [xpad[e, nd - x:nd - x + total, :].astype(jnp.bfloat16) for x in ds]
                left = left[0] if len(ds) == 1 else jnp.concatenate(left, axis=1)
                right = tiles[d] if len(ds) == 1 else jnp.concatenate([tiles[d], tiles[d + 1]], axis=0)
                acc = acc + jnp.dot(left, right, preferred_element_type=jnp.float32)
            results.append(acc.reshape(n, blocks, LANES))
        rs[:, pl.ds(start, 2 * blocks), :] = jnp.concatenate(results, axis=1).astype(jnp.bfloat16)

    for g in range(groups):
        for kind in forward:
            own(kind, g).wait()
            for k in order:
                arrival(kind, g, k).wait_recv()
        if sent_taps:
            rows = rows_of(TAPS, g)
            hf[:, rows, :] = hr[:, rows, :].astype(jnp.float32)

        def step(p, carry):
            one_pair(g * width, p)
            return carry

        lax.fori_loop(0, width // 2, step, 0)
        for k in order:
            remote(RESULT, g, k).start()
        own(RESULT, g).start()

    power[...] = jnp.zeros_like(power)
    for g in range(groups):
        own(RESULT, g).wait()
        for k in order:
            arrival(RESULT, g, k).wait_recv()

        def gather(d, carry):
            rows = rows_of(RESULT, g)
            at = pl.multiple_of(d * cl * blocks + g * width * blocks, width * blocks)
            piece = ogt[pl.ds(at, width * blocks), :] * cr[d, rows, :].astype(jnp.float32)
            mixed[pl.ds(at, width * blocks), :] = piece
            square = (piece * piece).reshape(width, blocks, LANES)
            power[...] += jnp.sum(square, axis=0)
            return carry

        lax.fori_loop(0, n, gather, 0)

    def exchange(k, incoming):
        other = source_of(mine, k, m) if incoming else peer_of(mine, k, m)
        return pltpu.make_async_remote_copy(
            src_ref=power,
            dst_ref=powers.at[other if incoming else mine],
            send_sem=psend_sem.at[k],
            recv_sem=precv_sem.at[k],
            device_id={"mp": other},
            device_id_type=MESH,
        )

    for k in range(1, m):
        exchange(k, False).start()
    for kind in forward + [RESULT]:
        for g in range(groups):
            for k in order:
                remote(kind, g, k).wait_send()
    for k in range(1, m):
        exchange(k, True).wait_recv()
    sums = power[...]
    for k in range(1, m):
        sums = sums + powers[source_of(mine, k, m)]
    scale = 1.0 / jnp.sqrt(sums / total_c + EPS)
    for a in range(blocks):
        part = mixed[pl.ds(a, channels, stride=blocks), :] * scale[a:a + 1, :]
        out[a * LANES:(a + 1) * LANES, :] = part.T.astype(jnp.bfloat16)
    for k in range(1, m):
        exchange(k, False).wait_send()


def solution(mesh):
    n, m = mesh.shape["seq"], mesh.shape["mp"]

    def local(gate_in, value_in, out_gate, filter_taps, skip_gain):
        tokens, channels = gate_in.shape
        blocks = tokens // LANES
        cl = channels // n
        width = min(cl, 8)
        groups = cl // width
        own_taps = filter_taps.shape[0]
        sent_taps = own_taps % LANES == 0 and (width * (own_taps // LANES)) % 16 == 0
        nd = own_taps * n // LANES
        if sent_taps:
            hs, he, taps = n, own_taps // LANES, filter_taps
        else:
            hs, he = 1, nd
            moved = lax.all_to_all(filter_taps, "seq", split_axis=1, concat_axis=0, tiled=True)
            taps = moved.astype(jnp.float32).T.reshape(1, cl * nd, LANES)
        cfg = (n, m, channels, blocks, cl, width, groups, sent_taps, hs, he, channels * m)
        vmem = pl.BlockSpec(memory_space=pltpu.VMEM)
        message = (n, cl * blocks, LANES)
        taps_message = (n, cl * he, LANES) if sent_taps else (n, 16, LANES)
        return pl.pallas_call(
            functools.partial(kernel, cfg),
            out_shape=jax.ShapeDtypeStruct((tokens, channels), jnp.bfloat16),
            in_specs=[vmem, vmem, vmem, vmem, pl.BlockSpec(memory_space=pltpu.SMEM)],
            out_specs=vmem,
            scratch_shapes=[
                pltpu.VMEM((channels * blocks, LANES), jnp.float32),
                pltpu.VMEM(message, jnp.bfloat16),
                pltpu.VMEM(taps_message, jnp.bfloat16),
                pltpu.VMEM(message, jnp.bfloat16),
                pltpu.VMEM(taps_message, jnp.bfloat16),
                pltpu.VMEM(taps_message, jnp.float32),
                pltpu.VMEM((2, nd + n * blocks, LANES), jnp.float32),
                pltpu.VMEM(message, jnp.bfloat16),
                pltpu.VMEM(message, jnp.bfloat16),
                pltpu.VMEM((channels * blocks, LANES), jnp.float32),
                pltpu.VMEM((channels * blocks, LANES), jnp.float32),
                pltpu.VMEM((blocks, LANES), jnp.float32),
                pltpu.VMEM((m, blocks, LANES), jnp.float32),
                pltpu.SemaphoreType.DMA((3, groups, n)),
                pltpu.SemaphoreType.DMA((3, groups, n)),
                pltpu.SemaphoreType.DMA((3, groups)),
                pltpu.SemaphoreType.DMA((m,)),
                pltpu.SemaphoreType.DMA((m,)),
            ],
            compiler_params=pltpu.CompilerParams(
                collective_id=0, has_side_effects=True, vmem_limit_bytes=48 * 1024 * 1024
            ),
        )(gate_in, value_in, out_gate, taps, skip_gain)

    return jax.shard_map(
        local,
        mesh=mesh,
        in_specs=(P("seq", "mp"), P("seq", "mp"), P("seq", "mp"), P("seq", "mp"), P("mp")),
        out_specs=P("seq", "mp"),
        check_vma=False,
    )
```

```python
import functools

import jax
import jax.numpy as jnp
from jax import lax
from jax.experimental import pallas as pl
from jax.experimental.pallas import tpu as pltpu
from jax.sharding import PartitionSpec as P

MESH = pl.DeviceIdType.MESH
LANES = 128
TAPS, GATED, RESULT = 0, 1, 2
EPS = 1e-05


def peer_of(me, k, n):
    if n & (n - 1) == 0:
        return me ^ k
    return lax.rem(me + k, n)


def source_of(me, k, n):
    if n & (n - 1) == 0:
        return me ^ k
    return lax.rem(me + n - k, n)


def kernel(cfg, gate_in, value_in, og_in, taps_in, skip_in, out, gate, value, og, taps, skip, stage,
           xm, hm, xr, hr, hf, xpad, rs, cr, ogt, mixed, power, powers, load_sem, send_sem, recv_sem,
           own_sem, psend_sem, precv_sem):
    n, m, channels, blocks, cl, width, groups, sent_taps, hs, he, total_c = cfg
    me = lax.axis_index("seq")
    mine = lax.axis_index("mp")
    nd = hs * he
    order = list(range(n - 1, 0, -1))

    loads = [
        pltpu.make_async_copy(src, dst, load_sem.at[i])
        for i, (src, dst) in enumerate(
            [(taps_in, taps), (gate_in, gate), (value_in, value), (og_in, og), (skip_in, skip)]
        )
    ]
    for load in loads:
        load.start()

    barrier = pltpu.get_barrier_semaphore()
    for k in range(1, n):
        pl.semaphore_signal(barrier, inc=1, device_id={"seq": peer_of(me, k, n)}, device_id_type=MESH)
    for k in range(1, m):
        pl.semaphore_signal(barrier, inc=1, device_id={"mp": peer_of(mine, k, m)}, device_id_type=MESH)

    loads[0].wait()
    if sent_taps:
        for e in range(he):
            part = taps[e * LANES:(e + 1) * LANES, :].astype(jnp.float32)
            stage[pl.ds(e, channels, stride=he), :] = part.T
        hm[...] = stage[: channels * he, :].astype(jnp.bfloat16).reshape(hm.shape)
    loads[1].wait()
    loads[2].wait()
    for a in range(blocks):
        span = slice(a * LANES, (a + 1) * LANES)
        part = gate[span, :].astype(jnp.float32) * value[span, :].astype(jnp.float32)
        stage[pl.ds(a, channels, stride=blocks), :] = part.T
    xm[...] = stage[...].astype(jnp.bfloat16).reshape(xm.shape)

    pl.semaphore_wait(barrier, n - 1 + m - 1)

    def rows_of(kind, g):
        per = he if kind == TAPS else blocks
        return pl.ds(g * width * per, width * per)

    def refs(kind):
        return {TAPS: (hm, hr), GATED: (xm, xr), RESULT: (rs, cr)}[kind]

    def remote(kind, g, k):
        src, dst = refs(kind)
        to = peer_of(me, k, n)
        rows = rows_of(kind, g)
        return pltpu.make_async_remote_copy(
            src_ref=src.at[to, rows],
            dst_ref=dst.at[me, rows],
            send_sem=send_sem.at[kind, g, k],
            recv_sem=recv_sem.at[kind, g, k],
            device_id={"seq": to},
            device_id_type=MESH,
        )

    def arrival(kind, g, k):
        src, dst = refs(kind)
        whence = source_of(me, k, n)
        rows = rows_of(kind, g)
        return pltpu.make_async_remote_copy(
            src_ref=src.at[whence, rows],
            dst_ref=dst.at[whence, rows],
            send_sem=send_sem.at[kind, g, k],
            recv_sem=recv_sem.at[kind, g, k],
            device_id={"seq": whence},
            device_id_type=MESH,
        )

    def own(kind, g):
        src, dst = refs(kind)
        rows = rows_of(kind, g)
        return pltpu.make_async_copy(src.at[me, rows], dst.at[me, rows], own_sem.at[kind, g])

    forward = ([TAPS] if sent_taps else []) + [GATED]
    for g in range(groups):
        for kind in forward:
            for k in order:
                remote(kind, g, k).start()
            own(kind, g).start()

    loads[3].wait()
    loads[4].wait()
    for a in range(blocks):
        span = slice(a * LANES, (a + 1) * LANES)
        ogt[pl.ds(a, channels, stride=blocks), :] = og[span, :].astype(jnp.float32).T
    xpad[:, :nd, :] = jnp.zeros((2, nd, LANES), jnp.float32)

    lane = lax.broadcasted_iota(jnp.int32, (16, LANES), 1)
    sub = lax.broadcasted_iota(jnp.int32, (16, LANES), 0)
    total = n * blocks

    def toeplitz(c):
        lines = []
        for d in range(nd):
            source = hf if sent_taps else taps
            line = source[d // he, pl.ds(c * he + d % he, 1), :]
            line = jnp.broadcast_to(line, (16, LANES))
            lines.append(pltpu.roll(line, 0, 1, stride=1, stride_axis=0))
        zero = jnp.zeros((16, LANES), jnp.float32)
        first = []
        for d in range(nd + 1):
            here = lines[d] if d < nd else zero
            before = lines[d - 1] if d > 0 else zero
            first.append(jnp.where(lane >= sub, here, before).astype(jnp.bfloat16))
        none = jnp.zeros((16, LANES), jnp.bfloat16)
        tiles = []
        turned = [[(f if q == 0 else pltpu.roll(f, 16 * q, 1)) for q in range(8)] for f in first]
        for d in range(nd + 1):
            rows = []
            for q in range(8):
                before = turned[d - 1][q] if d > 0 else none
                rows.append(turned[d][q] if q == 0 else jnp.where(lane >= 16 * q, turned[d][q], before))
            tiles.append(jnp.concatenate(rows, axis=0))
        return tiles

    def one_pair(base, p):
        c0 = base + 2 * p
        start = pl.multiple_of(c0 * blocks, 2 * blocks)
        both = xr[:, pl.ds(start, 2 * blocks), :].astype(jnp.float32)
        results = []
        for e in range(2):
            rows = both[:, e * blocks:(e + 1) * blocks, :].reshape(total, LANES)
            xpad[e, nd:, :] = rows
            tiles = toeplitz(c0 + e)
            acc = rows * skip[me * cl + c0 + e]
            for d in range(0, nd + 1, 2):
                ds = [d, d + 1] if d + 1 <= nd else [d]
                left = [xpad[e, nd - x:nd - x + total, :].astype(jnp.bfloat16) for x in ds]
                left = left[0] if len(ds) == 1 else jnp.concatenate(left, axis=1)
                right = tiles[d] if len(ds) == 1 else jnp.concatenate([tiles[d], tiles[d + 1]], axis=0)
                acc = acc + jnp.dot(left, right, preferred_element_type=jnp.float32)
            results.append(acc.reshape(n, blocks, LANES))
        rs[:, pl.ds(start, 2 * blocks), :] = jnp.concatenate(results, axis=1).astype(jnp.bfloat16)

    for g in range(groups):
        for kind in forward:
            own(kind, g).wait()
            for k in order:
                arrival(kind, g, k).wait_recv()
        if sent_taps:
            rows = rows_of(TAPS, g)
            hf[:, rows, :] = hr[:, rows, :].astype(jnp.float32)

        def step(p, carry):
            one_pair(g * width, p)
            return carry

        lax.fori_loop(0, width // 2, step, 0)
        for k in order:
            remote(RESULT, g, k).start()
        own(RESULT, g).start()

    power[...] = jnp.zeros_like(power)
    for g in range(groups):
        own(RESULT, g).wait()
        for k in order:
            arrival(RESULT, g, k).wait_recv()

        def gather(d, carry):
            rows = rows_of(RESULT, g)
            at = pl.multiple_of(d * cl * blocks + g * width * blocks, width * blocks)
            piece = ogt[pl.ds(at, width * blocks), :] * cr[d, rows, :].astype(jnp.float32)
            mixed[pl.ds(at, width * blocks), :] = piece
            square = (piece * piece).reshape(width, blocks, LANES)
            power[...] += jnp.sum(square, axis=0)
            return carry

        lax.fori_loop(0, n, gather, 0)

    def exchange(k, incoming):
        other = source_of(mine, k, m) if incoming else peer_of(mine, k, m)
        return pltpu.make_async_remote_copy(
            src_ref=power,
            dst_ref=powers.at[other if incoming else mine],
            send_sem=psend_sem.at[k],
            recv_sem=precv_sem.at[k],
            device_id={"mp": other},
            device_id_type=MESH,
        )

    for k in range(1, m):
        exchange(k, False).start()
    for kind in forward + [RESULT]:
        for g in range(groups):
            for k in order:
                remote(kind, g, k).wait_send()
    for k in range(1, m):
        exchange(k, True).wait_recv()
    sums = power[...]
    for k in range(1, m):
        sums = sums + powers[source_of(mine, k, m)]
    scale = 1.0 / jnp.sqrt(sums / total_c + EPS)
    for a in range(blocks):
        part = mixed[pl.ds(a, channels, stride=blocks), :] * scale[a:a + 1, :]
        out[a * LANES:(a + 1) * LANES, :] = part.T.astype(jnp.bfloat16)
    for k in range(1, m):
        exchange(k, False).wait_send()


def solution(mesh):
    n, m = mesh.shape["seq"], mesh.shape["mp"]

    def local(gate_in, value_in, out_gate, filter_taps, skip_gain):
        tokens, channels = gate_in.shape
        blocks = tokens // LANES
        cl = channels // n
        width = min(cl, 8)
        groups = cl // width
        own_taps = filter_taps.shape[0]
        sent_taps = own_taps % LANES == 0 and (width * (own_taps // LANES)) % 16 == 0
        nd = own_taps * n // LANES
        if sent_taps:
            hs, he, taps = n, own_taps // LANES, filter_taps
        else:
            hs, he = 1, nd
            moved = lax.all_to_all(filter_taps, "seq", split_axis=1, concat_axis=0, tiled=True)
            taps = moved.astype(jnp.float32).T.reshape(1, cl * nd, LANES)
        cfg = (n, m, channels, blocks, cl, width, groups, sent_taps, hs, he, channels * m)
        vmem = pl.BlockSpec(memory_space=pltpu.VMEM)
        message = (n, cl * blocks, LANES)
        taps_message = (n, cl * he, LANES) if sent_taps else (n, 16, LANES)
        return pl.pallas_call(
            functools.partial(kernel, cfg),
            out_shape=jax.ShapeDtypeStruct((tokens, channels), jnp.bfloat16),
            in_specs=[pl.BlockSpec(memory_space=pltpu.HBM)] * 5,
            out_specs=vmem,
            scratch_shapes=[
                pltpu.VMEM(gate_in.shape, gate_in.dtype),
                pltpu.VMEM(value_in.shape, value_in.dtype),
                pltpu.VMEM(out_gate.shape, out_gate.dtype),
                pltpu.VMEM(taps.shape, taps.dtype),
                pltpu.SMEM(skip_gain.shape, skip_gain.dtype),
                pltpu.VMEM((channels * blocks, LANES), jnp.float32),
                pltpu.VMEM(message, jnp.bfloat16),
                pltpu.VMEM(taps_message, jnp.bfloat16),
                pltpu.VMEM(message, jnp.bfloat16),
                pltpu.VMEM(taps_message, jnp.bfloat16),
                pltpu.VMEM(taps_message, jnp.float32),
                pltpu.VMEM((2, nd + n * blocks, LANES), jnp.float32),
                pltpu.VMEM(message, jnp.bfloat16),
                pltpu.VMEM(message, jnp.bfloat16),
                pltpu.VMEM((channels * blocks, LANES), jnp.float32),
                pltpu.VMEM((channels * blocks, LANES), jnp.float32),
                pltpu.VMEM((blocks, LANES), jnp.float32),
                pltpu.VMEM((m, blocks, LANES), jnp.float32),
                pltpu.SemaphoreType.DMA((5,)),
                pltpu.SemaphoreType.DMA((3, groups, n)),
                pltpu.SemaphoreType.DMA((3, groups, n)),
                pltpu.SemaphoreType.DMA((3, groups)),
                pltpu.SemaphoreType.DMA((m,)),
                pltpu.SemaphoreType.DMA((m,)),
            ],
            compiler_params=pltpu.CompilerParams(
                collective_id=0, has_side_effects=True, vmem_limit_bytes=67043328
            ),
        )(gate_in, value_in, out_gate, taps, skip_gain)

    return jax.shard_map(
        local,
        mesh=mesh,
        in_specs=(P("seq", "mp"), P("seq", "mp"), P("seq", "mp"), P("seq", "mp"), P("mp")),
        out_specs=P("seq", "mp"),
        check_vma=False,
    )
```
